32 devices in a mesh: chain: 16 (over z, y, x), grp: 2 (over core).
Axes of the slice: x: 2, y: 2, z: 4, core: 2. Of those that a mesh axis runs over, the one named last changes fastest.
Arguments:
- codes: bfloat16 [2, 16384, 6144], P(None, ('chain', 'grp')), may hold values from -6 to 6
- exponents: int32 [2, 512, 6144], P(None, ('chain', 'grp')), may hold values from -2 to 2
- column_map: int32 [32], replicated, may hold values from 0 to 31, each once
- row_order: int32 [32], replicated, may hold values from 0 to 31, each once
Outputs:
- rollout: bfloat16 [2, 6144, 16384], P(None, ('chain', 'grp'))
- block_sums: float32 [2, 6144, 512], P(None, ('chain', 'grp'))
The draws below stay inside these ranges and needn't reach their ends.
All inputs are finite; a program needn't handle non-finite values.
Results may differ from the reference program's by a relative error of at most 0.001.
Values may be sent and summed in bfloat16 or wider, within the bound.
A program may use at most 128 MiB of HBM per device.

```python
import jax
import jax.numpy as jnp

R = 16384
C = 6144
LAYERS = 2
N_CHAIN = 16
N_GRP = 2


def plant(result, key, low, largest):
    shape = result.shape
    place = [jax.random.randint(jax.random.fold_in(key, axis), (), 0, shape[axis]) for axis in range(len(shape))]
    result = result.at[tuple(place)].set(low)
    longest = shape.index(max(shape))
    place[longest] = (place[longest] + 1) % shape[longest]
    return result.at[tuple(place)].set(largest)


def block_levels(stream_key, extent, pieces, least, largest):
    def one(dim, parts):
        heights = jax.random.uniform(jax.random.fold_in(jax.random.fold_in(stream_key, 6), dim), (parts,), jnp.float32, least / len(pieces), largest / len(pieces))
        return jnp.repeat(jnp.exp(heights), extent[dim] // parts).reshape((-1,) + (1,) * (len(extent) - dim - 1))

    factor_of = one(*pieces[0])
    for cut in pieces[1:]:
        factor_of = factor_of * one(*cut)
    return factor_of


def gaussian(rng, shape, deviation, limit, shards=(), kind=jnp.bfloat16):
    result = jax.random.normal(rng, shape, jnp.float32) * deviation
    if len(shards) > 0:
        result = block_levels(rng, shape, shards, -0.22, 0.18) * result
    return jnp.clip(result, min=-limit, max=limit).astype(kind)


def setup_inputs(seed: int = 0) -> dict:
    arg_keys = jax.random.split(jax.random.key(seed), 5)
    return {
        "codes": gaussian(arg_keys[0], (LAYERS, R, C), 1.0, 6.0, ((1, 32),)),
        "exponents": plant(jax.random.randint(arg_keys[1], (LAYERS, R // 32, C), -2, 3), jax.random.fold_in(arg_keys[1], 1), -2, 2).astype(jnp.int32),
        "column_map": jax.random.permutation(arg_keys[2], N_CHAIN * N_GRP).astype(jnp.int32),
        "row_order": jax.random.permutation(arg_keys[3], N_CHAIN * N_GRP).astype(jnp.int32),
    }


def reference(codes, exponents, column_map, row_order):
    devices = N_CHAIN * N_GRP
    col_width = C // devices
    row_count = R // devices
    scaling = jnp.exp2(exponents.astype(jnp.float32))
    values = (codes.astype(jnp.float32) * jnp.repeat(scaling, 32, axis=1)).astype(jnp.bfloat16)
    col_index = (column_map[:, None] * col_width + jnp.arange(col_width, dtype=jnp.int32)[None, :]).reshape(-1)
    row_index = (row_order[:, None] * row_count + jnp.arange(row_count, dtype=jnp.int32)[None, :]).reshape(-1)
    picked = jnp.take(values, row_index.astype(jnp.int32), axis=1)
    picked = jnp.take(picked, col_index.astype(jnp.int32), axis=2)
    rollout = jnp.transpose(picked, (0, 2, 1))
    block_sums = rollout.astype(jnp.float32).reshape(LAYERS, C, R // 32, 32).sum(axis=-1)
    return rollout, block_sums
```

```python
import functools

import jax
import jax.numpy as jnp
from jax import lax
from jax.experimental import pallas as pl
from jax.experimental.pallas import tpu as pltpu
from jax.sharding import PartitionSpec as P

MESH = pl.DeviceIdType.MESH
BLOCK = 32
LANES = 128


def partner(me, step, devices):
    if devices & (devices - 1):
        return lax.rem(me + step, devices)
    peer, bit = 0, 1
    while bit < devices:
        peer = peer + lax.rem(me // bit + step // bit, 2) * bit
        bit *= 2
    return peer


def origin(me, step, devices):
    if devices & (devices - 1):
        return lax.rem(me - step + devices, devices)
    return partner(me, step, devices)


def turn_of(index, devices):
    if devices % 2:
        return index + 1
    odd = lax.rem(index, 2)
    return (index + odd) // 2 + (1 - odd) * (devices // 2)


class Traffic:
    def __init__(self, devices, grp_size, source, arrived, send_sems, recv_sems):
        self.devices, self.grp_size = devices, grp_size
        self.source, self.arrived = source, arrived
        self.send_sems, self.recv_sems = send_sems, recv_sems
        self.me = lax.axis_index("chain") * grp_size + lax.axis_index("grp")

    def copy(self, step, other, slot):
        return pltpu.make_async_remote_copy(
            src_ref=self.source(step, other),
            dst_ref=self.arrived.at[slot],
            send_sem=self.send_sems.at[step],
            recv_sem=self.recv_sems.at[step],
            device_id=(other // self.grp_size, lax.rem(other, self.grp_size)),
            device_id_type=MESH,
        )

    def send(self, step):
        return self.copy(step, partner(self.me, step, self.devices), self.me)

    def finish(self):
        @pl.loop(1, self.devices)
        def _(step):
            sender = origin(self.me, step, self.devices)
            self.copy(step, sender, sender).wait_recv()

        @pl.loop(1, self.devices)
        def _(step):
            self.send(step).wait_send()


def fused_kernel(
    devices, grp_size, column_map, codes, exponents, arrived,
    codes_in, exponents_in, turned, sending, load_sems, send_sems, recv_sems,
):
    pairs, layers, rows, pair = codes_in.shape
    col_width = pair // 2

    def loads(index):
        columns = pl.ds(pl.multiple_of(index * pair, LANES), pair)
        return (
            pltpu.make_async_copy(codes.at[:, :, columns], codes_in.at[index], load_sems.at[0, index]),
            pltpu.make_async_copy(exponents.at[:, :, columns], exponents_in.at[index], load_sems.at[1, index]),
        )

    @pl.loop(0, pairs)
    def _(index):
        for load in loads(index):
            load.start()

    @pl.loop(0, pairs)
    def _(index):
        for load in loads(index):
            load.wait()

    traffic = Traffic(
        devices, grp_size, lambda step, other: sending.at[step], arrived, send_sems, recv_sems
    )

    def fill(step):
        column = column_map[partner(traffic.me, step, devices)]
        which = column // 2
        for layer in range(layers):
            scaling = jnp.exp2(exponents_in[which, layer].astype(jnp.float32)).astype(jnp.bfloat16)
            for first in range(0, rows, LANES):
                pieces = []
                for row in range(first, first + LANES, BLOCK):
                    block = row // BLOCK
                    values = codes_in[which, layer, row : row + BLOCK, :]
                    pieces.append(values * scaling[block : block + 1, :])
                both = jnp.concatenate(pieces, axis=0).T
                turned[0, layer, :, first : first + LANES] = both[:col_width]
                turned[1, layer, :, first : first + LANES] = both[col_width:]
        sending[step] = turned[lax.rem(column, 2)]

    fill(turn_of(0, devices))

    @pl.loop(1, devices - 1)
    def _(index):
        fill(turn_of(index, devices))
        traffic.send(turn_of(index - 1, devices)).start()

    fill(0)
    traffic.send(turn_of(devices - 2, devices)).start()
    arrived[traffic.me] = sending[0]
    traffic.finish()


def exchange_kernel(devices, grp_size, outgoing, arrived, own, send_sems, recv_sems, own_sems):
    traffic = Traffic(
        devices, grp_size, lambda step, other: outgoing.at[other], arrived, send_sems, recv_sems
    )

    @pl.loop(0, devices - 1)
    def _(index):
        traffic.send(turn_of(index, devices)).start()

    take = pltpu.make_async_copy(outgoing.at[traffic.me], own, own_sems.at[0])
    take.start()
    take.wait()
    put = pltpu.make_async_copy(own, arrived.at[traffic.me], own_sems.at[1])
    put.start()
    put.wait()
    traffic.finish()


def exchange(codes, exponents, column_map, devices, grp_size):
    layers, rows, width = codes.shape
    col_width = width // devices
    block = (layers, col_width, rows)
    shape = jax.ShapeDtypeStruct((devices, *block), jnp.bfloat16)
    anywhere = pl.BlockSpec(memory_space=pl.ANY)
    peers = pltpu.SemaphoreType.DMA((devices,))
    if col_width % 64 or rows % LANES or devices % 2:
        scaling = jnp.exp2(exponents.astype(jnp.float32))
        values = (codes.astype(jnp.float32) * jnp.repeat(scaling, BLOCK, axis=1)).astype(jnp.bfloat16)
        values = values.reshape(layers, rows, devices, col_width)
        outgoing = jnp.take(values.transpose(2, 0, 3, 1), column_map, axis=0)
        return pl.pallas_call(
            functools.partial(exchange_kernel, devices, grp_size),
            out_shape=shape,
            in_specs=[anywhere],
            out_specs=anywhere,
            scratch_shapes=[pltpu.VMEM(block, jnp.bfloat16), peers, peers, pltpu.SemaphoreType.DMA((2,))],
            compiler_params=pltpu.CompilerParams(has_side_effects=True),
        )(outgoing)
    pairs = devices // 2
    return pl.pallas_call(
        functools.partial(fused_kernel, devices, grp_size),
        out_shape=pltpu.VMEM((devices, *block), jnp.bfloat16),
        in_specs=[pl.BlockSpec(memory_space=pltpu.SMEM), anywhere, anywhere],
        out_specs=pl.BlockSpec(memory_space=pltpu.VMEM),
        scratch_shapes=[
            pltpu.VMEM((pairs, layers, rows, 2 * col_width), codes.dtype),
            pltpu.VMEM((pairs, layers, rows // BLOCK, 2 * col_width), exponents.dtype),
            pltpu.VMEM((2, *block), jnp.bfloat16),
            pltpu.VMEM((devices, *block), jnp.bfloat16),
            pltpu.SemaphoreType.DMA((2, pairs)),
            peers,
            peers,
        ],
        compiler_params=pltpu.CompilerParams(has_side_effects=True, vmem_limit_bytes=44 << 20),
    )(column_map, codes, exponents)


def deliver_kernel(order, arrived, rollout, sums, sums_out, block_sems, sums_sem):
    devices, layers, col_width, rows = arrived.shape
    blocks = rows // BLOCK
    count = LANES // blocks

    def place(slot):
        columns = pl.ds(pl.multiple_of(slot * rows, LANES), rows)
        return pltpu.make_async_copy(arrived.at[order[slot]], rollout.at[:, :, columns], block_sems.at[slot])

    @pl.loop(0, devices)
    def _(slot):
        place(slot).start()

    row_block = lax.broadcasted_iota(jnp.int32, (rows, LANES), 0) // BLOCK
    column = lax.broadcasted_iota(jnp.int32, (rows, LANES), 1)
    choosers = [
        jnp.where(column == row_block + part * blocks, 1.0, 0.0).astype(jnp.bfloat16) for part in range(count)
    ]

    for group in range(devices // count):
        for layer in range(layers):
            total = None
            for part in range(count):
                values = arrived[order[group * count + part], layer]
                term = jnp.dot(values, choosers[part], preferred_element_type=jnp.float32)
                total = term if total is None else total + term
            sums_out[layer, :, group * LANES : (group + 1) * LANES] = total

    out = pltpu.make_async_copy(sums_out, sums, sums_sem)
    out.start()

    @pl.loop(0, devices)
    def _(slot):
        place(slot).wait()

    out.wait()


def finish(arrived, row_order):
    devices, layers, col_width, rows = arrived.shape
    blocks = rows // BLOCK
    count = max(1, LANES // blocks)
    if rows % LANES or blocks * count != LANES or devices % count or col_width % 16:
        rollout = jnp.take(arrived, row_order, axis=0).transpose(1, 2, 0, 3)
        rollout = rollout.reshape(layers, col_width, devices * rows)
        sums = rollout.astype(jnp.float32).reshape(layers, col_width, devices * blocks, BLOCK).sum(axis=-1)
        return rollout, sums
    sums_shape = (layers, col_width, devices * blocks)
    anywhere = pl.BlockSpec(memory_space=pl.ANY)
    arrived = pltpu.with_memory_space_constraint(arrived, pltpu.VMEM)
    return pl.pallas_call(
        deliver_kernel,
        out_shape=[
            jax.ShapeDtypeStruct((layers, col_width, devices * rows), jnp.bfloat16),
            jax.ShapeDtypeStruct(sums_shape, jnp.float32),
        ],
        in_specs=[pl.BlockSpec(memory_space=pltpu.SMEM), pl.BlockSpec(memory_space=pltpu.VMEM)],
        out_specs=[anywhere, anywhere],
        scratch_shapes=[
            pltpu.VMEM(sums_shape, jnp.float32),
            pltpu.SemaphoreType.DMA((devices,)),
            pltpu.SemaphoreType.DMA,
        ],
        compiler_params=pltpu.CompilerParams(vmem_limit_bytes=16 << 20),
    )(row_order, arrived)


def shards(codes, exponents, column_map, row_order):
    grp_size = lax.axis_size("grp")
    devices = lax.axis_size("chain") * grp_size
    arrived = exchange(codes, exponents, column_map, devices, grp_size)
    rollout, sums = finish(arrived, row_order)
    return (rollout, sums)


def solution(mesh):
    return jax.shard_map(
        shards,
        mesh=mesh,
        in_specs=(P(None, ("chain", "grp"), None), P(None, ("chain", "grp"), None), P(), P()),
        out_specs=(P(None, ("chain", "grp"), None), P(None, ("chain", "grp"), None)),
        check_vma=False,
    )
```

```python
import functools

import jax
import jax.numpy as jnp
from jax import lax
from jax.experimental import pallas as pl
from jax.experimental.pallas import tpu as pltpu
from jax.sharding import PartitionSpec as P

MESH = pl.DeviceIdType.MESH
BLOCK = 32
LANES = 128
EARLY = 2


def partner(me, step, devices):
    if devices & (devices - 1):
        return lax.rem(me + step, devices)
    peer, bit = 0, 1
    while bit < devices:
        peer = peer + lax.rem(me // bit + step // bit, 2) * bit
        bit *= 2
    return peer


def origin(me, step, devices):
    if devices & (devices - 1):
        return lax.rem(me - step + devices, devices)
    return partner(me, step, devices)


def turn_of(index, devices):
    half = devices // 2
    return jnp.where(index < devices - half, index + half, index - (devices - half) + 1)


class Traffic:
    def __init__(self, devices, grp_size, pieces, source, arrived, send_sems, recv_sems):
        self.devices, self.grp_size, self.pieces = devices, grp_size, pieces
        self.source, self.arrived = source, arrived
        self.send_sems, self.recv_sems = send_sems, recv_sems
        self.me = lax.axis_index("chain") * grp_size + lax.axis_index("grp")

    def place(self, other):
        return (other // self.grp_size, lax.rem(other, self.grp_size))

    def copy(self, step, piece, other, slot):
        return pltpu.make_async_remote_copy(
            src_ref=self.source(step, piece, other),
            dst_ref=self.arrived.at[slot] if self.pieces == 1 else self.arrived.at[slot, piece],
            send_sem=self.send_sems.at[step, piece],
            recv_sem=self.recv_sems.at[step, piece],
            device_id=self.place(other),
            device_id_type=MESH,
        )

    def send(self, step, piece):
        return self.copy(step, piece, partner(self.me, step, self.devices), self.me)

    def greet(self):
        barrier = pltpu.get_barrier_semaphore()

        @pl.loop(1, self.devices)
        def _(step):
            other = self.place(partner(self.me, step, self.devices))
            pl.semaphore_signal(barrier, inc=1, device_id=other, device_id_type=MESH)

    def greeted(self):
        pl.semaphore_wait(pltpu.get_barrier_semaphore(), self.devices - 1)

    def finish(self):
        @pl.loop(1, self.devices)
        def _(step):
            sender = origin(self.me, step, self.devices)
            for piece in range(self.pieces):
                self.copy(step, piece, sender, sender).wait_recv()

        @pl.loop(1, self.devices)
        def _(step):
            for piece in range(self.pieces):
                self.send(step, piece).wait_send()


def fused_kernel(devices, grp_size, layers, column_map_in, row_order_in, codes, exponents, arrived, row_order, column_map, map_sem, order_sem, *scratch):
    codes_in, exponents_in = scratch[:layers], scratch[layers : 2 * layers]
    turned, sending, load_sems, send_sems, recv_sems = scratch[2 * layers :]
    pairs, rows, pair = codes_in[0].shape
    col_width = pair // 2
    traffic = Traffic(
        devices, grp_size, layers, lambda step, piece, other: sending.at[step, piece], arrived, send_sems, recv_sems
    )

    def loads(layer, index):
        columns = pl.ds(pl.multiple_of(index * pair, LANES), pair)
        return (
            pltpu.make_async_copy(
                exponents.at[layer, :, columns], exponents_in[layer].at[index], load_sems.at[0, layer, index]
            ),
            pltpu.make_async_copy(codes.at[layer, :, columns], codes_in[layer].at[index], load_sems.at[1, layer, index]),
        )

    def start_loads(layer):
        @pl.loop(0, pairs)
        def _(index):
            for load in loads(layer, index):
                load.start()

    def wait_loads(layer):
        @pl.loop(0, pairs)
        def _(index):
            for load in loads(layer, index):
                load.wait()

    def fill(step, layer, out):
        column = column_map[partner(traffic.me, step, devices)]
        which = column // 2
        scaling = jnp.exp2(exponents_in[layer][which].astype(jnp.float32)).astype(jnp.bfloat16)
        for first in range(0, rows, LANES):
            pieces = []
            for row in range(first, first + LANES, BLOCK):
                block = row // BLOCK
                values = codes_in[layer][which, row : row + BLOCK, :]
                pieces.append(values * scaling[block : block + 1, :])
            both = jnp.concatenate(pieces, axis=0).T
            turned[0, :, first : first + LANES] = both[:col_width]
            turned[1, :, first : first + LANES] = both[col_width:]
        out[...] = turned[lax.rem(column, 2)]

    def prepare(index, layer):
        step = turn_of(index, devices)
        fill(step, layer, sending.at[step, layer])

    def send(index, layer):
        traffic.send(turn_of(index, devices), layer).start()

    def send_before(index, layer):
        if layer:
            send(index, layer - 1)
        else:
            send(index - 1, layers - 1)

    early = min(EARLY, devices - 1)
    mapping = pltpu.make_async_copy(column_map_in, column_map, map_sem)
    mapping.start()
    ordering = pltpu.make_async_copy(row_order_in, row_order, order_sem)
    ordering.start()
    start_loads(0)
    traffic.greet()
    mapping.wait()
    ordering.wait()
    wait_loads(0)
    for layer in range(1, layers):
        start_loads(layer)

    @pl.loop(0, early)
    def _(index):
        prepare(index, 0)

    traffic.greeted()

    @pl.loop(0, early - 1)
    def _(index):
        send(index, 0)

    for layer in range(1, layers):
        wait_loads(layer)

        @pl.loop(0, early)
        def _(index):
            prepare(index, layer)

    send(early - 1, 0)
    for layer in range(1, layers):

        @pl.loop(0, early - (1 if layer == layers - 1 else 0))
        def _(index):
            send(index, layer)

    @pl.loop(early, devices - 1)
    def _(index):
        for layer in range(layers):
            prepare(index, layer)
            send_before(index, layer)

    for layer in range(layers):
        fill(0, layer, arrived.at[traffic.me, layer])
        if layer == 0:
            send(devices - 2, layers - 1)
    traffic.finish()


def exchange_kernel(devices, grp_size, outgoing, arrived, own, send_sems, recv_sems, own_sems):
    traffic = Traffic(
        devices, grp_size, 1, lambda step, piece, other: outgoing.at[other], arrived, send_sems, recv_sems
    )
    traffic.greet()
    traffic.greeted()

    @pl.loop(0, devices - 1)
    def _(index):
        traffic.send(turn_of(index, devices), 0).start()

    take = pltpu.make_async_copy(outgoing.at[traffic.me], own, own_sems.at[0])
    take.start()
    take.wait()
    put = pltpu.make_async_copy(own, arrived.at[traffic.me], own_sems.at[1])
    put.start()
    put.wait()
    traffic.finish()


def exchange(codes, exponents, column_map, row_order, devices, grp_size):
    layers, rows, width = codes.shape
    col_width = width // devices
    block = (layers, col_width, rows)
    anywhere = pl.BlockSpec(memory_space=pl.ANY)
    if col_width % 64 or rows % LANES or devices % 2:
        scaling = jnp.exp2(exponents.astype(jnp.float32))
        values = (codes.astype(jnp.float32) * jnp.repeat(scaling, BLOCK, axis=1)).astype(jnp.bfloat16)
        values = values.reshape(layers, rows, devices, col_width)
        outgoing = jnp.take(values.transpose(2, 0, 3, 1), column_map, axis=0)
        peers = pltpu.SemaphoreType.DMA((devices, 1))
        return pl.pallas_call(
            functools.partial(exchange_kernel, devices, grp_size),
            out_shape=jax.ShapeDtypeStruct((devices, *block), jnp.bfloat16),
            in_specs=[anywhere],
            out_specs=anywhere,
            scratch_shapes=[pltpu.VMEM(block, jnp.bfloat16), peers, peers, pltpu.SemaphoreType.DMA((2,))],
            compiler_params=pltpu.CompilerParams(has_side_effects=True, collective_id=0),
        )(outgoing), row_order
    peers = pltpu.SemaphoreType.DMA((devices, layers))
    return pl.pallas_call(
        functools.partial(fused_kernel, devices, grp_size, layers),
        out_shape=[
            pltpu.VMEM((devices, *block), jnp.bfloat16),
            pltpu.SMEM(row_order.shape, row_order.dtype),
        ],
        in_specs=[anywhere] * 4,
        out_specs=[pl.BlockSpec(memory_space=pltpu.VMEM), pl.BlockSpec(memory_space=pltpu.SMEM)],
        scratch_shapes=[
            pltpu.SMEM(column_map.shape, column_map.dtype),
            pltpu.SemaphoreType.DMA,
            pltpu.SemaphoreType.DMA,
            *[pltpu.VMEM((devices // 2, rows, 2 * col_width), codes.dtype)] * layers,
            *[pltpu.VMEM((devices // 2, rows // BLOCK, 2 * col_width), exponents.dtype)] * layers,
            pltpu.VMEM((2, col_width, rows), jnp.bfloat16),
            pltpu.VMEM((devices, *block), jnp.bfloat16),
            pltpu.SemaphoreType.DMA((2, layers, devices // 2)),
            peers,
            peers,
        ],
        compiler_params=pltpu.CompilerParams(
            has_side_effects=True, collective_id=0, vmem_limit_bytes=44 << 20
        ),
    )(column_map, row_order, codes, exponents)


def deliver_kernel(order, arrived, rollout, sums, sums_out, block_sems, sums_sem):
    devices, layers, col_width, rows = arrived.shape
    blocks = rows // BLOCK
    count = LANES // blocks

    def place(slot):
        columns = pl.ds(pl.multiple_of(slot * rows, LANES), rows)
        return pltpu.make_async_copy(arrived.at[order[slot]], rollout.at[:, :, columns], block_sems.at[slot])

    @pl.loop(0, devices)
    def _(slot):
        place(slot).start()

    row_block = lax.broadcasted_iota(jnp.int32, (rows, LANES), 0) // BLOCK
    column = lax.broadcasted_iota(jnp.int32, (rows, LANES), 1)
    choosers = [
        jnp.where(column == row_block + part * blocks, 1.0, 0.0).astype(jnp.bfloat16) for part in range(count)
    ]

    for group in range(devices // count):
        for layer in range(layers):
            total = None
            for part in range(count):
                values = arrived[order[group * count + part], layer]
                term = jnp.dot(values, choosers[part], preferred_element_type=jnp.float32)
                total = term if total is None else total + term
            sums_out[layer, :, group * LANES : (group + 1) * LANES] = total

    out = pltpu.make_async_copy(sums_out, sums, sums_sem)
    out.start()

    @pl.loop(0, devices)
    def _(slot):
        place(slot).wait()

    out.wait()


def finish(arrived, row_order):
    devices, layers, col_width, rows = arrived.shape
    blocks = rows // BLOCK
    count = max(1, LANES // blocks)
    if rows % LANES or blocks * count != LANES or devices % count or col_width % 16:
        rollout = jnp.take(arrived, row_order, axis=0).transpose(1, 2, 0, 3)
        rollout = rollout.reshape(layers, col_width, devices * rows)
        sums = rollout.astype(jnp.float32).reshape(layers, col_width, devices * blocks, BLOCK).sum(axis=-1)
        return rollout, sums
    sums_shape = (layers, col_width, devices * blocks)
    anywhere = pl.BlockSpec(memory_space=pl.ANY)
    arrived = pltpu.with_memory_space_constraint(arrived, pltpu.VMEM)
    row_order = pltpu.with_memory_space_constraint(row_order, pltpu.SMEM)
    return pl.pallas_call(
        deliver_kernel,
        out_shape=[
            jax.ShapeDtypeStruct((layers, col_width, devices * rows), jnp.bfloat16),
            jax.ShapeDtypeStruct(sums_shape, jnp.float32),
        ],
        in_specs=[pl.BlockSpec(memory_space=pltpu.SMEM), pl.BlockSpec(memory_space=pltpu.VMEM)],
        out_specs=[anywhere, anywhere],
        scratch_shapes=[
            pltpu.VMEM(sums_shape, jnp.float32),
            pltpu.SemaphoreType.DMA((devices,)),
            pltpu.SemaphoreType.DMA,
        ],
        compiler_params=pltpu.CompilerParams(vmem_limit_bytes=16 << 20),
    )(row_order, arrived)


def shards(codes, exponents, column_map, row_order):
    grp_size = lax.axis_size("grp")
    devices = lax.axis_size("chain") * grp_size
    arrived, order = exchange(codes, exponents, column_map, row_order, devices, grp_size)
    rollout, sums = finish(arrived, order)
    return (rollout, sums)


def solution(mesh):
    return jax.shard_map(
        shards,
        mesh=mesh,
        in_specs=(P(None, ("chain", "grp"), None), P(None, ("chain", "grp"), None), P(), P()),
        out_specs=(P(None, ("chain", "grp"), None), P(None, ("chain", "grp"), None)),
        check_vma=False,
    )
```

```python
import functools

import jax
import jax.numpy as jnp
from jax import lax
from jax.experimental import pallas as pl
from jax.experimental.pallas import tpu as pltpu
from jax.sharding import PartitionSpec as P

MESH = pl.DeviceIdType.MESH
BLOCK = 32
LANES = 128


def turn_of(index, devices):
    half = devices // 2
    return jnp.where(index < devices - half, index + half, index - (devices - half) + 1)


class Traffic:
    def __init__(self, devices, grp_size, pieces, source, arrived, send_sems, recv_sems):
        self.devices, self.grp_size, self.pieces = devices, grp_size, pieces
        self.source, self.arrived = source, arrived
        self.send_sems, self.recv_sems = send_sems, recv_sems
        self.me = lax.axis_index("chain") * grp_size + lax.axis_index("grp")
        self.flips = []
        bit = 1
        while bit < devices and not devices & (devices - 1):
            self.flips.append((bit, bit - 2 * bit * lax.rem(self.me // bit, 2)))
            bit *= 2

    def partner(self, step):
        if not self.flips:
            return lax.rem(self.me + step, self.devices)
        if isinstance(step, int):
            return self.me + sum(flip for bit, flip in self.flips if step & bit)
        return self.me + sum(lax.rem(step // bit, 2) * flip for bit, flip in self.flips)

    def origin(self, step):
        return self.partner(step) if self.flips else lax.rem(self.me - step + self.devices, self.devices)

    def place(self, other):
        return (other // self.grp_size, lax.rem(other, self.grp_size))

    def copy(self, step, piece, other, slot):
        return pltpu.make_async_remote_copy(
            src_ref=self.source(step, piece, other),
            dst_ref=self.arrived.at[slot] if self.pieces == 1 else self.arrived.at[slot, piece],
            send_sem=self.send_sems.at[step, piece],
            recv_sem=self.recv_sems.at[step, piece],
            device_id=self.place(other),
            device_id_type=MESH,
        )

    def send(self, step, piece):
        return self.copy(step, piece, self.partner(step), self.me)

    def greet(self):
        barrier = pltpu.get_barrier_semaphore()

        for step in range(1, self.devices):
            other = self.place(self.partner(step))
            pl.semaphore_signal(barrier, inc=1, device_id=other, device_id_type=MESH)

    def greeted(self):
        pl.semaphore_wait(pltpu.get_barrier_semaphore(), self.devices - 1)

    def finish(self):
        @pl.loop(1, self.devices)
        def _(step):
            sender = self.origin(step)
            for piece in range(self.pieces):
                self.send(step, piece).wait_send()
                self.copy(step, piece, sender, sender).wait_recv()


def fused_kernel(
    devices, grp_size, layers, column_map_in, row_order_in, codes, exponents, arrived, row_order, column_map, *scratch
):
    codes_in, exponents_in, scalings = (scratch[group * layers : (group + 1) * layers] for group in range(3))
    turned, sending, map_sems, load_sems, send_sems, recv_sems = scratch[3 * layers :]
    pairs, rows, pair = codes_in[0].shape
    col_width = pair // 2
    traffic = Traffic(
        devices, grp_size, layers, lambda step, piece, other: sending.at[step, piece], arrived, send_sems, recv_sems
    )

    def columns_of(index):
        return pl.ds(index * pair, pair)

    def loads(layer):
        yield pltpu.make_async_copy(exponents.at[layer], exponents_in[layer], load_sems.at[layer, pairs])
        for index in range(pairs):
            source = codes.at[layer, :, columns_of(index)]
            yield pltpu.make_async_copy(source, codes_in[layer].at[index], load_sems.at[layer, index])

    def loaded(layer):
        for load in loads(layer):
            load.wait()
        for index in range(pairs):
            powers = jnp.exp2(exponents_in[layer][:, columns_of(index)].astype(jnp.float32))
            scalings[layer][index] = powers.astype(jnp.bfloat16)

    def fill(step, layer, out):
        column = column_map[traffic.partner(step)]
        which = column // 2
        scaling = scalings[layer][which]
        for first in range(0, rows, LANES):
            pieces = []
            for row in range(first, first + LANES, BLOCK):
                block = row // BLOCK
                values = codes_in[layer][which, row : row + BLOCK, :]
                pieces.append(values * scaling[block : block + 1, :])
            both = jnp.concatenate(pieces, axis=0).T
            turned[0, :, first : first + LANES] = both[:col_width]
            turned[1, :, first : first + LANES] = both[col_width:]
        out[...] = turned[lax.rem(column, 2)]

    def prepare(index, layer):
        step = turn_of(index, devices)
        fill(step, layer, sending.at[step, layer])

    def send(index, layer):
        traffic.send(turn_of(index, devices), layer).start()

    mapping = pltpu.make_async_copy(column_map_in, column_map, map_sems.at[0])
    ordering = pltpu.make_async_copy(row_order_in, row_order, map_sems.at[1])
    mapping.start()
    traffic.greet()
    for load in loads(0):
        load.start()
    ordering.start()
    mapping.wait()
    loaded(0)
    for layer in range(1, layers):
        for load in loads(layer):
            load.start()
    prepare(0, 0)
    prepare(1, 0)
    traffic.greeted()
    send(0, 0)
    for layer in range(1, layers):
        loaded(layer)
        for index in range(2):
            prepare(index, layer)
            send(1 - index, layer - 1 + index)
    ordering.wait()

    @pl.loop(2, devices - 1)
    def _(index):
        for layer in range(layers):
            prepare(index, layer)
            if layer:
                send(index, layer - 1)
            else:
                send(index - 1, layers - 1)

    for layer in range(layers):
        fill(0, layer, arrived.at[traffic.me, layer])
        if layer == 0:
            send(devices - 2, layers - 1)
    traffic.finish()


def exchange_kernel(devices, grp_size, outgoing, arrived, own, send_sems, recv_sems, own_sems):
    traffic = Traffic(
        devices, grp_size, 1, lambda step, piece, other: outgoing.at[other], arrived, send_sems, recv_sems
    )
    traffic.greet()
    traffic.greeted()

    @pl.loop(0, devices - 1)
    def _(index):
        traffic.send(turn_of(index, devices), 0).start()

    take = pltpu.make_async_copy(outgoing.at[traffic.me], own, own_sems.at[0])
    take.start()
    take.wait()
    put = pltpu.make_async_copy(own, arrived.at[traffic.me], own_sems.at[1])
    put.start()
    put.wait()
    traffic.finish()


def exchange(codes, exponents, column_map, row_order, devices, grp_size):
    layers, rows, width = codes.shape
    col_width = width // devices
    block = (layers, col_width, rows)
    anywhere = pl.BlockSpec(memory_space=pl.ANY)
    if col_width % 64 or rows % LANES or devices % 2:
        scaling = jnp.exp2(exponents.astype(jnp.float32))
        values = (codes.astype(jnp.float32) * jnp.repeat(scaling, BLOCK, axis=1)).astype(jnp.bfloat16)
        values = values.reshape(layers, rows, devices, col_width)
        outgoing = jnp.take(values.transpose(2, 0, 3, 1), column_map, axis=0)
        peers = pltpu.SemaphoreType.DMA((devices, 1))
        return pl.pallas_call(
            functools.partial(exchange_kernel, devices, grp_size),
            out_shape=jax.ShapeDtypeStruct((devices, *block), jnp.bfloat16),
            in_specs=[anywhere],
            out_specs=anywhere,
            scratch_shapes=[pltpu.VMEM(block, jnp.bfloat16), peers, peers, pltpu.SemaphoreType.DMA((2,))],
            compiler_params=pltpu.CompilerParams(has_side_effects=True, collective_id=0),
        )(outgoing), row_order
    peers = pltpu.SemaphoreType.DMA((devices, layers))
    return pl.pallas_call(
        functools.partial(fused_kernel, devices, grp_size, layers),
        out_shape=[
            pltpu.VMEM((devices, *block), jnp.bfloat16),
            pltpu.SMEM(row_order.shape, row_order.dtype),
        ],
        in_specs=[anywhere] * 4,
        out_specs=[pl.BlockSpec(memory_space=pltpu.VMEM), pl.BlockSpec(memory_space=pltpu.SMEM)],
        scratch_shapes=[
            pltpu.SMEM(column_map.shape, column_map.dtype),
            *[pltpu.VMEM((devices // 2, rows, 2 * col_width), codes.dtype)] * layers,
            *[pltpu.VMEM((rows // BLOCK, width), exponents.dtype)] * layers,
            *[pltpu.VMEM((devices // 2, rows // BLOCK, 2 * col_width), jnp.bfloat16)] * layers,
            pltpu.VMEM((2, col_width, rows), jnp.bfloat16),
            pltpu.VMEM((devices, *block), jnp.bfloat16),
            pltpu.SemaphoreType.DMA((2,)),
            pltpu.SemaphoreType.DMA((layers, devices // 2 + 1)),
            peers,
            peers,
        ],
        compiler_params=pltpu.CompilerParams(
            has_side_effects=True, collective_id=0, vmem_limit_bytes=44 << 20
        ),
    )(column_map, row_order, codes, exponents)


def deliver_kernel(order, arrived, rollout, sums, sums_out, block_sems, sums_sem):
    devices, layers, col_width, rows = arrived.shape
    blocks = rows // BLOCK
    count = LANES // blocks

    def place(slot):
        columns = pl.ds(pl.multiple_of(slot * rows, LANES), rows)
        return pltpu.make_async_copy(arrived.at[order[slot]], rollout.at[:, :, columns], block_sems.at[slot])

    @pl.loop(0, devices)
    def _(slot):
        place(slot).start()

    row_block = lax.broadcasted_iota(jnp.int32, (rows, LANES), 0) // BLOCK
    column = lax.broadcasted_iota(jnp.int32, (rows, LANES), 1)
    choosers = [
        jnp.where(column == row_block + part * blocks, 1.0, 0.0).astype(jnp.bfloat16) for part in range(count)
    ]

    for group in range(devices // count):
        for layer in range(layers):
            total = None
            for part in range(count):
                values = arrived[order[group * count + part], layer]
                term = jnp.dot(values, choosers[part], preferred_element_type=jnp.float32)
                total = term if total is None else total + term
            sums_out[layer, :, group * LANES : (group + 1) * LANES] = total

    out = pltpu.make_async_copy(sums_out, sums, sums_sem)
    out.start()

    @pl.loop(0, devices)
    def _(slot):
        place(slot).wait()

    out.wait()


def finish(arrived, row_order):
    devices, layers, col_width, rows = arrived.shape
    blocks = rows // BLOCK
    count = max(1, LANES // blocks)
    if rows % LANES or blocks * count != LANES or devices % count or col_width % 16:
        rollout = jnp.take(arrived, row_order, axis=0).transpose(1, 2, 0, 3)
        rollout = rollout.reshape(layers, col_width, devices * rows)
        sums = rollout.astype(jnp.float32).reshape(layers, col_width, devices * blocks, BLOCK).sum(axis=-1)
        return rollout, sums
    sums_shape = (layers, col_width, devices * blocks)
    anywhere = pl.BlockSpec(memory_space=pl.ANY)
    arrived = pltpu.with_memory_space_constraint(arrived, pltpu.VMEM)
    row_order = pltpu.with_memory_space_constraint(row_order, pltpu.SMEM)
    return pl.pallas_call(
        deliver_kernel,
        out_shape=[
            jax.ShapeDtypeStruct((layers, col_width, devices * rows), jnp.bfloat16),
            jax.ShapeDtypeStruct(sums_shape, jnp.float32),
        ],
        in_specs=[pl.BlockSpec(memory_space=pltpu.SMEM), pl.BlockSpec(memory_space=pltpu.VMEM)],
        out_specs=[anywhere, anywhere],
        scratch_shapes=[
            pltpu.VMEM(sums_shape, jnp.float32),
            pltpu.SemaphoreType.DMA((devices,)),
            pltpu.SemaphoreType.DMA,
        ],
        compiler_params=pltpu.CompilerParams(vmem_limit_bytes=16 << 20),
    )(row_order, arrived)


def shards(codes, exponents, column_map, row_order):
    grp_size = lax.axis_size("grp")
    devices = lax.axis_size("chain") * grp_size
    arrived, order = exchange(codes, exponents, column_map, row_order, devices, grp_size)
    rollout, sums = finish(arrived, order)
    return (rollout, sums)


def solution(mesh):
    return jax.shard_map(
        shards,
        mesh=mesh,
        in_specs=(P(None, ("chain", "grp"), None), P(None, ("chain", "grp"), None), P(), P()),
        out_specs=(P(None, ("chain", "grp"), None), P(None, ("chain", "grp"), None)),
        check_vma=False,
    )
```

```python
import functools

import jax
import jax.numpy as jnp
from jax import lax
from jax.experimental import pallas as pl
from jax.experimental.pallas import tpu as pltpu
from jax.sharding import PartitionSpec as P

MESH = pl.DeviceIdType.MESH
BLOCK = 32
LANES = 128


def turn_of(index, devices):
    half = devices // 2
    return jnp.where(index < devices - half, index + half, index - (devices - half) + 1)


class Traffic:
    def __init__(self, devices, grp_size, pieces, source, arrived, send_sem, recv_sem):
        self.devices, self.grp_size, self.pieces = devices, grp_size, pieces
        self.source, self.arrived = source, arrived
        self.send_sem, self.recv_sem = send_sem, recv_sem
        self.me = lax.axis_index("chain") * grp_size + lax.axis_index("grp")
        self.flips = []
        bit = 1
        while bit < devices and not devices & (devices - 1):
            self.flips.append((bit, bit - 2 * bit * lax.rem(self.me // bit, 2)))
            bit *= 2

    def partner(self, step):
        if not self.flips:
            return lax.rem(self.me + step, self.devices)
        if isinstance(step, int):
            return self.me + sum(flip for bit, flip in self.flips if step & bit)
        return self.me + sum(lax.rem(step // bit, 2) * flip for bit, flip in self.flips)

    def origin(self, step):
        return self.partner(step) if self.flips else lax.rem(self.me - step + self.devices, self.devices)

    def place(self, other):
        return (other // self.grp_size, lax.rem(other, self.grp_size))

    def copy(self, step, piece, other, slot):
        return pltpu.make_async_remote_copy(
            src_ref=self.source(step, piece, other),
            dst_ref=self.arrived.at[slot] if self.pieces == 1 else self.arrived.at[slot, piece],
            send_sem=self.send_sem,
            recv_sem=self.recv_sem,
            device_id=self.place(other),
            device_id_type=MESH,
        )

    def send(self, step, piece):
        return self.copy(step, piece, self.partner(step), self.me)

    def greet(self):
        barrier = pltpu.get_barrier_semaphore()

        for step in range(1, self.devices):
            other = self.place(self.partner(step))
            pl.semaphore_signal(barrier, inc=1, device_id=other, device_id_type=MESH)

    def greeted(self):
        pl.semaphore_wait(pltpu.get_barrier_semaphore(), self.devices - 1)

    def finish(self, blocks):
        every = pl.ds(0, self.devices - 1)
        total = pltpu.make_async_remote_copy(
            src_ref=blocks.at[every],
            dst_ref=self.arrived.at[every],
            send_sem=self.send_sem,
            recv_sem=self.recv_sem,
            device_id=self.place(self.partner(1)),
            device_id_type=MESH,
        )
        total.wait_send()
        total.wait_recv()


def fused_kernel(
    devices, grp_size, layers, column_map_in, row_order_in, codes, exponents, arrived, row_order, column_map, *scratch
):
    codes_in, exponents_in, scalings = (scratch[group * layers : (group + 1) * layers] for group in range(3))
    turned, sending, map_sems, load_sems, send_sem, recv_sem = scratch[3 * layers :]
    pairs, rows, pair = codes_in[0].shape
    col_width = pair // 2
    traffic = Traffic(
        devices, grp_size, layers, lambda step, piece, other: sending.at[step, piece], arrived, send_sem, recv_sem
    )

    def columns_of(index):
        return pl.ds(index * pair, pair)

    def start_loads(layer):
        pltpu.make_async_copy(exponents.at[layer], exponents_in[layer], load_sems.at[layer, 0]).start()
        for index in range(pairs):
            source = codes.at[layer, :, columns_of(index)]
            pltpu.make_async_copy(source, codes_in[layer].at[index], load_sems.at[layer, 1]).start()

    def loaded(layer):
        pltpu.make_async_copy(exponents.at[layer], exponents_in[layer], load_sems.at[layer, 0]).wait()
        for index in range(pairs):
            powers = jnp.exp2(exponents_in[layer][:, columns_of(index)].astype(jnp.float32))
            scalings[layer][index] = powers.astype(jnp.bfloat16)
        pltpu.make_async_copy(codes_in[layer], codes_in[layer], load_sems.at[layer, 1]).wait()

    def fill(step, layer, out):
        column = column_map[traffic.partner(step)]
        which = column // 2
        scaling = scalings[layer][which]
        for first in range(0, rows, LANES):
            pieces = []
            for row in range(first, first + LANES, BLOCK):
                block = row // BLOCK
                values = codes_in[layer][which, row : row + BLOCK, :]
                pieces.append(values * scaling[block : block + 1, :])
            both = jnp.concatenate(pieces, axis=0).T
            turned[0, :, first : first + LANES] = both[:col_width]
            turned[1, :, first : first + LANES] = both[col_width:]
        out[...] = turned[lax.rem(column, 2)]

    def prepare(index, layer):
        step = turn_of(index, devices)
        fill(step, layer, sending.at[step, layer])

    def send(index, layer):
        traffic.send(turn_of(index, devices), layer).start()

    mapping = pltpu.make_async_copy(column_map_in, column_map, map_sems.at[0])
    ordering = pltpu.make_async_copy(row_order_in, row_order, map_sems.at[1])
    mapping.start()
    traffic.greet()
    start_loads(0)
    ordering.start()
    mapping.wait()
    loaded(0)
    for layer in range(1, layers):
        start_loads(layer)
    prepare(0, 0)
    prepare(1, 0)
    traffic.greeted()
    send(0, 0)
    for layer in range(1, layers):
        loaded(layer)
        for index in range(2):
            prepare(index, layer)
            send(1 - index, layer - 1 + index)
    ordering.wait()

    @pl.loop(2, devices - 1)
    def _(index):
        for layer in range(layers):
            prepare(index, layer)
            if layer:
                send(index, layer - 1)
            else:
                send(index - 1, layers - 1)

    for layer in range(layers):
        fill(0, layer, arrived.at[traffic.me, layer])
        if layer == 0:
            send(devices - 2, layers - 1)
    traffic.finish(sending)


def exchange_kernel(devices, grp_size, outgoing, arrived, own, send_sem, recv_sem, own_sems):
    traffic = Traffic(
        devices, grp_size, 1, lambda step, piece, other: outgoing.at[other], arrived, send_sem, recv_sem
    )
    traffic.greet()
    traffic.greeted()

    @pl.loop(0, devices - 1)
    def _(index):
        traffic.send(turn_of(index, devices), 0).start()

    take = pltpu.make_async_copy(outgoing.at[traffic.me], own, own_sems.at[0])
    take.start()
    take.wait()
    put = pltpu.make_async_copy(own, arrived.at[traffic.me], own_sems.at[1])
    put.start()
    put.wait()
    traffic.finish(outgoing)


def exchange(codes, exponents, column_map, row_order, devices, grp_size):
    layers, rows, width = codes.shape
    col_width = width // devices
    block = (layers, col_width, rows)
    anywhere = pl.BlockSpec(memory_space=pl.ANY)
    if col_width % 64 or rows % LANES or devices % 2:
        scaling = jnp.exp2(exponents.astype(jnp.float32))
        values = (codes.astype(jnp.float32) * jnp.repeat(scaling, BLOCK, axis=1)).astype(jnp.bfloat16)
        values = values.reshape(layers, rows, devices, col_width)
        outgoing = jnp.take(values.transpose(2, 0, 3, 1), column_map, axis=0)
        return pl.pallas_call(
            functools.partial(exchange_kernel, devices, grp_size),
            out_shape=jax.ShapeDtypeStruct((devices, *block), jnp.bfloat16),
            in_specs=[anywhere],
            out_specs=anywhere,
            scratch_shapes=[
                pltpu.VMEM(block, jnp.bfloat16),
                *[pltpu.SemaphoreType.DMA] * 2,
                pltpu.SemaphoreType.DMA((2,)),
            ],
            compiler_params=pltpu.CompilerParams(has_side_effects=True, collective_id=0),
        )(outgoing), row_order
    return pl.pallas_call(
        functools.partial(fused_kernel, devices, grp_size, layers),
        out_shape=[
            pltpu.VMEM((devices, *block), jnp.bfloat16),
            pltpu.SMEM(row_order.shape, row_order.dtype),
        ],
        in_specs=[anywhere] * 4,
        out_specs=[pl.BlockSpec(memory_space=pltpu.VMEM), pl.BlockSpec(memory_space=pltpu.SMEM)],
        scratch_shapes=[
            pltpu.SMEM(column_map.shape, column_map.dtype),
            *[pltpu.VMEM((devices // 2, rows, 2 * col_width), codes.dtype)] * layers,
            *[pltpu.VMEM((rows // BLOCK, width), exponents.dtype)] * layers,
            *[pltpu.VMEM((devices // 2, rows // BLOCK, 2 * col_width), jnp.bfloat16)] * layers,
            pltpu.VMEM((2, col_width, rows), jnp.bfloat16),
            pltpu.VMEM((devices, *block), jnp.bfloat16),
            pltpu.SemaphoreType.DMA((2,)),
            pltpu.SemaphoreType.DMA((layers, 2)),
            *[pltpu.SemaphoreType.DMA] * 2,
        ],
        compiler_params=pltpu.CompilerParams(
            has_side_effects=True, collective_id=0, vmem_limit_bytes=44 << 20
        ),
    )(column_map, row_order, codes, exponents)


def deliver_kernel(order, arrived, rollout, sums, sums_out, blocks_sem, sums_sem):
    devices, layers, col_width, rows = arrived.shape
    blocks = rows // BLOCK
    count = LANES // blocks

    def place(slot):
        columns = pl.ds(pl.multiple_of(slot * rows, LANES), rows)
        return pltpu.make_async_copy(arrived.at[order[slot]], rollout.at[:, :, columns], blocks_sem)

    @pl.loop(0, devices)
    def _(slot):
        place(slot).start()

    row_block = lax.broadcasted_iota(jnp.int32, (rows, LANES), 0) // BLOCK
    column = lax.broadcasted_iota(jnp.int32, (rows, LANES), 1)
    choosers = [
        jnp.where(column == row_block + part * blocks, 1.0, 0.0).astype(jnp.bfloat16) for part in range(count)
    ]

    for group in range(devices // count):
        for layer in range(layers):
            total = None
            for part in range(count):
                values = arrived[order[group * count + part], layer]
                term = jnp.dot(values, choosers[part], preferred_element_type=jnp.float32)
                total = term if total is None else total + term
            sums_out[layer, :, group * LANES : (group + 1) * LANES] = total

    out = pltpu.make_async_copy(sums_out, sums, sums_sem)
    out.start()

    pltpu.make_async_copy(rollout, rollout, blocks_sem).wait()
    out.wait()


def finish(arrived, row_order):
    devices, layers, col_width, rows = arrived.shape
    blocks = rows // BLOCK
    count = max(1, LANES // blocks)
    if rows % LANES or blocks * count != LANES or devices % count or col_width % 16:
        rollout = jnp.take(arrived, row_order, axis=0).transpose(1, 2, 0, 3)
        rollout = rollout.reshape(layers, col_width, devices * rows)
        sums = rollout.astype(jnp.float32).reshape(layers, col_width, devices * blocks, BLOCK).sum(axis=-1)
        return rollout, sums
    sums_shape = (layers, col_width, devices * blocks)
    anywhere = pl.BlockSpec(memory_space=pl.ANY)
    arrived = pltpu.with_memory_space_constraint(arrived, pltpu.VMEM)
    row_order = pltpu.with_memory_space_constraint(row_order, pltpu.SMEM)
    return pl.pallas_call(
        deliver_kernel,
        out_shape=[
            jax.ShapeDtypeStruct((layers, col_width, devices * rows), jnp.bfloat16),
            jax.ShapeDtypeStruct(sums_shape, jnp.float32),
        ],
        in_specs=[pl.BlockSpec(memory_space=pltpu.SMEM), pl.BlockSpec(memory_space=pltpu.VMEM)],
        out_specs=[anywhere, anywhere],
        scratch_shapes=[
            pltpu.VMEM(sums_shape, jnp.float32),
            pltpu.SemaphoreType.DMA,
            pltpu.SemaphoreType.DMA,
        ],
        compiler_params=pltpu.CompilerParams(vmem_limit_bytes=16 << 20),
    )(row_order, arrived)


def shards(codes, exponents, column_map, row_order):
    grp_size = lax.axis_size("grp")
    devices = lax.axis_size("chain") * grp_size
    arrived, order = exchange(codes, exponents, column_map, row_order, devices, grp_size)
    rollout, sums = finish(arrived, order)
    return (rollout, sums)


def solution(mesh):
    return jax.shard_map(
        shards,
        mesh=mesh,
        in_specs=(P(None, ("chain", "grp"), None), P(None, ("chain", "grp"), None), P(), P()),
        out_specs=(P(None, ("chain", "grp"), None), P(None, ("chain", "grp"), None)),
        check_vma=False,
    )
```

```python
import functools

import jax
import jax.numpy as jnp
from jax import lax
from jax.experimental import pallas as pl
from jax.experimental.pallas import tpu as pltpu
from jax.sharding import PartitionSpec as P

MESH = pl.DeviceIdType.MESH
BLOCK = 32
LANES = 128


def turn_of(index, devices):
    half = devices // 2
    return jnp.where(index < devices - half, index + half, index - (devices - half) + 1)


class Traffic:
    def __init__(self, devices, grp_size, pieces, source, arrived, send_sem, recv_sem):
        self.devices, self.grp_size, self.pieces = devices, grp_size, pieces
        self.source, self.arrived = source, arrived
        self.send_sem, self.recv_sem = send_sem, recv_sem
        self.me = lax.axis_index("chain") * grp_size + lax.axis_index("grp")
        self.flips = []
        bit = 1
        while bit < devices and not devices & (devices - 1):
            self.flips.append((bit, bit - 2 * bit * lax.rem(self.me // bit, 2)))
            bit *= 2

    def partner(self, step):
        if not self.flips:
            return lax.rem(self.me + step, self.devices)
        if isinstance(step, int):
            return self.me + sum(flip for bit, flip in self.flips if step & bit)
        return self.me + sum(lax.rem(step // bit, 2) * flip for bit, flip in self.flips)

    def origin(self, step):
        return self.partner(step) if self.flips else lax.rem(self.me - step + self.devices, self.devices)

    def place(self, other):
        return (other // self.grp_size, lax.rem(other, self.grp_size))

    def copy(self, step, piece, other, slot):
        return pltpu.make_async_remote_copy(
            src_ref=self.source(step, piece, other),
            dst_ref=self.arrived.at[slot] if self.pieces == 1 else self.arrived.at[slot, piece],
            send_sem=self.send_sem,
            recv_sem=self.recv_sem,
            device_id=self.place(other),
            device_id_type=MESH,
        )

    def send(self, step, piece):
        return self.copy(step, piece, self.partner(step), self.me)

    def greet(self):
        barrier = pltpu.get_barrier_semaphore()

        for step in range(1, self.devices):
            other = self.place(self.partner(step))
            pl.semaphore_signal(barrier, inc=1, device_id=other, device_id_type=MESH)

    def greeted(self):
        pl.semaphore_wait(pltpu.get_barrier_semaphore(), self.devices - 1)

    def finish(self, blocks):
        every = pl.ds(0, self.devices - 1)
        total = pltpu.make_async_remote_copy(
            src_ref=blocks.at[every],
            dst_ref=self.arrived.at[every],
            send_sem=self.send_sem,
            recv_sem=self.recv_sem,
            device_id=self.place(self.partner(1)),
            device_id_type=MESH,
        )
        total.wait_send()
        total.wait_recv()


def fused_kernel(
    devices, grp_size, layers, column_map_in, row_order_in, codes, exponents, arrived, row_order, column_map, *scratch
):
    codes_in, exponents_in, scalings = (scratch[group * layers : (group + 1) * layers] for group in range(3))
    turned, sending, map_sems, load_sems, send_sem, recv_sem = scratch[3 * layers :]
    pairs, rows, pair = codes_in[0].shape
    col_width = pair // 2
    traffic = Traffic(
        devices, grp_size, layers, lambda step, piece, other: sending.at[step, piece], arrived, send_sem, recv_sem
    )

    def columns_of(index):
        return pl.ds(index * pair, pair)

    def start_loads(layer):
        pltpu.make_async_copy(exponents.at[layer], exponents_in[layer], load_sems.at[layer, 0]).start()
        for index in range(pairs):
            source = codes.at[layer, :, columns_of(index)]
            pltpu.make_async_copy(source, codes_in[layer].at[index], load_sems.at[layer, 1]).start()

    def loaded(layer):
        pltpu.make_async_copy(exponents.at[layer], exponents_in[layer], load_sems.at[layer, 0]).wait()
        for index in range(pairs):
            powers = jnp.exp2(exponents_in[layer][:, columns_of(index)].astype(jnp.float32))
            scalings[layer][index] = powers.astype(jnp.bfloat16)
        pltpu.make_async_copy(codes_in[layer], codes_in[layer], load_sems.at[layer, 1]).wait()

    def fill(step, layer, out):
        column = column_map[traffic.partner(step)]
        which = column // 2
        scaling = scalings[layer][which]
        for first in range(0, rows, LANES):
            pieces = []
            for row in range(first, first + LANES, BLOCK):
                block = row // BLOCK
                values = codes_in[layer][which, row : row + BLOCK, :]
                pieces.append(values * scaling[block : block + 1, :])
            both = jnp.concatenate(pieces, axis=0).T
            turned[0, :, first : first + LANES] = both[:col_width]
            turned[1, :, first : first + LANES] = both[col_width:]
        out[...] = turned[lax.rem(column, 2)]

    def prepare(index, layer):
        step = turn_of(index, devices)
        fill(step, layer, sending.at[step, layer])

    def send(index, layer):
        traffic.send(turn_of(index, devices), layer).start()

    mapping = pltpu.make_async_copy(column_map_in, column_map, map_sems.at[0])
    ordering = pltpu.make_async_copy(row_order_in, row_order, map_sems.at[1])
    mapping.start()
    traffic.greet()
    start_loads(0)
    ordering.start()
    mapping.wait()
    loaded(0)
    prepare(0, 0)
    prepare(1, 0)
    traffic.greeted()
    send(0, 0)
    for layer in range(1, layers):
        start_loads(layer)
    for layer in range(1, layers):
        loaded(layer)
        for index in range(2):
            prepare(index, layer)
            send(1 - index, layer - 1 + index)
    ordering.wait()

    @pl.loop(2, devices - 1)
    def _(index):
        for layer in range(layers):
            prepare(index, layer)
            if layer:
                send(index, layer - 1)
            else:
                send(index - 1, layers - 1)

    for layer in range(layers):
        fill(0, layer, arrived.at[traffic.me, layer])
        if layer == 0:
            send(devices - 2, layers - 1)
    traffic.finish(sending)


def exchange_kernel(devices, grp_size, outgoing, arrived, own, send_sem, recv_sem, own_sems):
    traffic = Traffic(
        devices, grp_size, 1, lambda step, piece, other: outgoing.at[other], arrived, send_sem, recv_sem
    )
    traffic.greet()
    traffic.greeted()

    @pl.loop(0, devices - 1)
    def _(index):
        traffic.send(turn_of(index, devices), 0).start()

    take = pltpu.make_async_copy(outgoing.at[traffic.me], own, own_sems.at[0])
    take.start()
    take.wait()
    put = pltpu.make_async_copy(own, arrived.at[traffic.me], own_sems.at[1])
    put.start()
    put.wait()
    traffic.finish(outgoing)


def exchange(codes, exponents, column_map, row_order, devices, grp_size):
    layers, rows, width = codes.shape
    col_width = width // devices
    block = (layers, col_width, rows)
    anywhere = pl.BlockSpec(memory_space=pl.ANY)
    if col_width % 64 or rows % LANES or devices % 2:
        scaling = jnp.exp2(exponents.astype(jnp.float32))
        values = (codes.astype(jnp.float32) * jnp.repeat(scaling, BLOCK, axis=1)).astype(jnp.bfloat16)
        values = values.reshape(layers, rows, devices, col_width)
        outgoing = jnp.take(values.transpose(2, 0, 3, 1), column_map, axis=0)
        return pl.pallas_call(
            functools.partial(exchange_kernel, devices, grp_size),
            out_shape=jax.ShapeDtypeStruct((devices, *block), jnp.bfloat16),
            in_specs=[anywhere],
            out_specs=anywhere,
            scratch_shapes=[
                pltpu.VMEM(block, jnp.bfloat16),
                *[pltpu.SemaphoreType.DMA] * 2,
                pltpu.SemaphoreType.DMA((2,)),
            ],
            compiler_params=pltpu.CompilerParams(has_side_effects=True, collective_id=0),
        )(outgoing), row_order
    return pl.pallas_call(
        functools.partial(fused_kernel, devices, grp_size, layers),
        out_shape=[
            pltpu.VMEM((devices, *block), jnp.bfloat16),
            pltpu.SMEM(row_order.shape, row_order.dtype),
        ],
        in_specs=[anywhere] * 4,
        out_specs=[pl.BlockSpec(memory_space=pltpu.VMEM), pl.BlockSpec(memory_space=pltpu.SMEM)],
        scratch_shapes=[
            pltpu.SMEM(column_map.shape, column_map.dtype),
            *[pltpu.VMEM((devices // 2, rows, 2 * col_width), codes.dtype)] * layers,
            *[pltpu.VMEM((rows // BLOCK, width), exponents.dtype)] * layers,
            *[pltpu.VMEM((devices // 2, rows // BLOCK, 2 * col_width), jnp.bfloat16)] * layers,
            pltpu.VMEM((2, col_width, rows), jnp.bfloat16),
            pltpu.VMEM((devices, *block), jnp.bfloat16),
            pltpu.SemaphoreType.DMA((2,)),
            pltpu.SemaphoreType.DMA((layers, 2)),
            *[pltpu.SemaphoreType.DMA] * 2,
        ],
        compiler_params=pltpu.CompilerParams(
            has_side_effects=True, collective_id=0, vmem_limit_bytes=44 << 20
        ),
    )(column_map, row_order, codes, exponents)


def deliver_kernel(order, arrived, rollout, sums, sums_out, blocks_sem, sums_sem):
    devices, layers, col_width, rows = arrived.shape
    blocks = rows // BLOCK
    count = LANES // blocks

    def place(slot):
        columns = pl.ds(pl.multiple_of(slot * rows, LANES), rows)
        return pltpu.make_async_copy(arrived.at[order[slot]], rollout.at[:, :, columns], blocks_sem)

    @pl.loop(0, devices)
    def _(slot):
        place(slot).start()

    row_block = lax.broadcasted_iota(jnp.int32, (rows, LANES), 0) // BLOCK
    column = lax.broadcasted_iota(jnp.int32, (rows, LANES), 1)
    choosers = [
        jnp.where(column == row_block + part * blocks, 1.0, 0.0).astype(jnp.bfloat16) for part in range(count)
    ]

    for group in range(devices // count):
        for layer in range(layers):
            total = None
            for part in range(count):
                values = arrived[order[group * count + part], layer]
                term = jnp.dot(values, choosers[part], preferred_element_type=jnp.float32)
                total = term if total is None else total + term
            sums_out[layer, :, group * LANES : (group + 1) * LANES] = total

    out = pltpu.make_async_copy(sums_out, sums, sums_sem)
    out.start()

    pltpu.make_async_copy(rollout, rollout, blocks_sem).wait()
    out.wait()


def finish(arrived, row_order):
    devices, layers, col_width, rows = arrived.shape
    blocks = rows // BLOCK
    count = max(1, LANES // blocks)
    if rows % LANES or blocks * count != LANES or devices % count or col_width % 16:
        rollout = jnp.take(arrived, row_order, axis=0).transpose(1, 2, 0, 3)
        rollout = rollout.reshape(layers, col_width, devices * rows)
        sums = rollout.astype(jnp.float32).reshape(layers, col_width, devices * blocks, BLOCK).sum(axis=-1)
        return rollout, sums
    sums_shape = (layers, col_width, devices * blocks)
    anywhere = pl.BlockSpec(memory_space=pl.ANY)
    arrived = pltpu.with_memory_space_constraint(arrived, pltpu.VMEM)
    row_order = pltpu.with_memory_space_constraint(row_order, pltpu.SMEM)
    return pl.pallas_call(
        deliver_kernel,
        out_shape=[
            jax.ShapeDtypeStruct((layers, col_width, devices * rows), jnp.bfloat16),
            jax.ShapeDtypeStruct(sums_shape, jnp.float32),
        ],
        in_specs=[pl.BlockSpec(memory_space=pltpu.SMEM), pl.BlockSpec(memory_space=pltpu.VMEM)],
        out_specs=[anywhere, anywhere],
        scratch_shapes=[
            pltpu.VMEM(sums_shape, jnp.float32),
            pltpu.SemaphoreType.DMA,
            pltpu.SemaphoreType.DMA,
        ],
        compiler_params=pltpu.CompilerParams(vmem_limit_bytes=16 << 20),
    )(row_order, arrived)


def shards(codes, exponents, column_map, row_order):
    grp_size = lax.axis_size("grp")
    devices = lax.axis_size("chain") * grp_size
    arrived, order = exchange(codes, exponents, column_map, row_order, devices, grp_size)
    rollout, sums = finish(arrived, order)
    return (rollout, sums)


def solution(mesh):
    return jax.shard_map(
        shards,
        mesh=mesh,
        in_specs=(P(None, ("chain", "grp"), None), P(None, ("chain", "grp"), None), P(), P()),
        out_specs=(P(None, ("chain", "grp"), None), P(None, ("chain", "grp"), None)),
        check_vma=False,
    )
```
